32 devices in a mesh: groups: 2 (over y), tm: 4 (over z), chan: 4 (over x, core).
Axes of the slice: x: 2, y: 2, z: 4, core: 2. Of those that a mesh axis runs over, the one named last changes fastest.
Arguments:
- vis: bfloat16 [8, 128, 2, 128], P(('groups', 'chan'), 'tm'), parts along dimension 0, may hold values from -6 to 6
- row_weight: bfloat16 [8, 128, 128, 128], P(('groups', 'chan'), 'tm'), parts along dimension 0, may hold values from -4 to 4
- col_weight: bfloat16 [8, 128, 128, 256], P(('groups', 'chan'), 'tm'), parts along dimension 0, may hold values from -0.5 to 0.5
- w_bin: int32 [8, 128, 1], P(('groups', 'chan'), 'tm'), parts along dimension 0, may hold values from 0 to 3; in each aligned block of 32 rows (0 to 31, 32 to 63, ..., all dimensions but the last counted through in order) at most 16 rows name the same one
- tile_col: int32 [8, 128], P(('groups', 'chan'), 'tm'), parts along dimension 0, may hold values from 0 to 15
- w_kernel: bfloat16 [8, 512, 512], P(('groups', 'tm')), parts along dimension 0, may hold values from -0.25 to 0.25
Outputs:
- grid: float32 [8, 128, 16, 512], P(('groups', 'tm'), 'chan'), parts along dimension 0
The draws below stay inside these ranges and needn't reach their ends.
There are 2 independent parts, one for each index of `groups`. The reference program is written for one: setup_inputs(seed, part) draws one part's arguments, and reference() takes and returns one part's arrays. A program takes and returns all parts, laid end to end along the dimension named above; each array names one. Nothing has to cross between parts.
Inputs may be any that keep to these rules, and one draw needn't show every extreme that they name: `w_bin`: within the blocks of one device (aligned blocks of 32 along the channel-group and block dimensions taken together), no w-plane is named more than 16 times, a bound that some block reaches.
All inputs are finite; a program needn't handle non-finite values.
Results may differ from the reference program's by a relative error of at most 0.0041.
Values may be sent and summed in bfloat16 or wider, within the bound.
A program may use at most 128 MiB of HBM per device.

```python
import math
import jax
import jax.numpy as jnp
import numpy as np
from jax import lax

VIS = 128
KROWS = 128
QW = 256
BLK_DEV = 32
TC = 16
NW = 4
BLOCKS = 128
CHANS = 4
CAP = 16


def touch_ends(drawn, stream_key, smallest, top_value):
    spot = [jax.random.randint(jax.random.fold_in(stream_key, axis), (), 0, length) for axis, length in enumerate(drawn.shape)]
    longest = drawn.shape.index(max(drawn.shape))
    next_to = spot[:longest] + [(spot[longest] + 1) % drawn.shape[longest]] + spot[longest + 1:]
    return drawn.at[tuple(spot)].set(smallest).at[tuple(next_to)].set(top_value)


def steps_of(own_key, extent, cuts, low, high):
    def one(dim, blocks):
        steps = jax.random.uniform(jax.random.fold_in(jax.random.fold_in(own_key, 6), dim), (blocks,), jnp.float32, low / len(cuts), high / len(cuts))
        return jnp.repeat(jnp.exp(steps), extent[dim] // blocks).reshape((-1,) + (1,) * (len(extent) - dim - 1))

    level = one(*cuts[0])
    for cut in cuts[1:]:
        level = level * one(*cut)
    return level


def deal_out(rng, own, number, rows, count, top, most, skew):
    ranking = jax.random.permutation(rng, count)
    crowded, ordinary = portions_of(count, rows * top, most, skew, True), portions_of(count, rows * top, most, skew, False)
    places = jnp.arange(count)

    def named(lengths, turn):
        used = int((lengths > 0).sum())
        fixed = max(1, used // 4)
        moved = fixed + (places - fixed + turn * (used - fixed)) % max(1, count - fixed)
        return jnp.zeros((count,), jnp.int32).at[ranking[jnp.where(places < fixed, places, moved)]].set(jnp.asarray(lengths, jnp.int32))

    lengths = jnp.where(number % 4 == 0, named(crowded, number // 4), named(ordinary, number - number // 4 - 1))
    mixed = jax.random.permutation(jax.random.fold_in(own, 3), count)
    source_of, taker = mixed[0:count // 2 * 2:2], mixed[1:count // 2 * 2:2]
    margin = jnp.minimum(lengths[source_of] - 1, most - lengths[taker]) // 2
    margin = jnp.where((source_of == ranking[0]) | (taker == ranking[0]) | (lengths[taker] == 0), 0, jnp.maximum(margin, 0))
    moved = jax.random.randint(jax.random.fold_in(own, 4), (count // 2,), 0, 1 << 20) % (margin + 1)
    lengths = lengths.at[source_of].add(-moved).at[taker].add(moved)
    items = jnp.searchsorted(jnp.cumsum(lengths), jnp.arange(rows * top), side="right").astype(jnp.int32)
    table = items.reshape(top, rows).T
    table = table[jax.random.permutation(jax.random.fold_in(own, 1), rows)]
    turn = jax.random.randint(jax.random.fold_in(own, 2), (rows, 1), 0, top)
    return jnp.take_along_axis(table, (jnp.arange(top)[None, :] + turn) % top, axis=1)


def portions_of(number_of, total, most, skew, full):
    weights = [(1 << 20) // math.isqrt(grade ** skew) + 1 for grade in range(1, number_of + 1)]
    largest = most if full else min(most, max(-(-total // number_of), total * weights[0] // sum(weights)))
    least = 1 if total - largest >= number_of - 1 else 0
    given, spare = [largest] + [least] * (number_of - 1), total - largest - least * (number_of - 1)
    while spare > 0:
        candidates = [i for i in range(1, number_of) if given[i] < largest] or [i for i in range(1, number_of) if given[i] < most]
        whole, left = sum([weights[i] for i in candidates]), spare
        for i in candidates:
            extra = min(most - given[i], max(1, left * weights[i] // whole), spare)
            given[i] = given[i] + extra
            spare = spare - extra
    return np.array(given)


def gaussian(own_key, shape, width, reach, shards=(), held_as=jnp.bfloat16):
    loudness = steps_of(own_key, shape, shards, -0.22, 0.18) if shards else 1.0
    array = jax.random.normal(own_key, shape, jnp.float32) * width * loudness
    return jnp.minimum(jnp.maximum(array, -reach), reach).astype(held_as)


def setup_inputs(seed: int = 0, part: int = 0) -> dict:
    seeds = jax.random.split(jax.random.key(seed), 7)
    part_keys = jax.random.split(jax.random.fold_in(seeds[6], part), 7)
    vis = gaussian(part_keys[0], (CHANS, BLOCKS, 2, VIS), 1.0, 6.0, ((0, 4), (1, 4)))
    row_weight = gaussian(part_keys[1], (CHANS, BLOCKS, KROWS, VIS), 0.25, 4.0, ((0, 4), (1, 4)))
    col_weight = gaussian(part_keys[2], (CHANS, BLOCKS, VIS, QW), VIS ** -0.5, 0.5, ((0, 4), (1, 4)))
    w_bin_keys = jax.random.split(jax.random.fold_in(part_keys[3], 1), CHANS * BLOCKS // BLK_DEV)
    w_bin_turns = jax.random.permutation(jax.random.fold_in(part_keys[3], 3), CHANS * BLOCKS // BLK_DEV)
    w_bin = jax.vmap(lambda own, number: deal_out(jax.random.fold_in(part_keys[3], 2), own, number, BLK_DEV, NW, 1, CAP, 2))(w_bin_keys, w_bin_turns).reshape((CHANS, BLOCKS, 1))
    tile_col = touch_ends(jax.random.randint(part_keys[4], (CHANS, BLOCKS), 0, TC), jax.random.fold_in(part_keys[4], 1), 0, TC - 1).astype(jnp.int32)
    w_kernel = gaussian(part_keys[5], (NW, 2 * QW, 2 * QW), (2 * QW) ** -0.5, 0.25, ((0, 4),))
    return {"vis": vis, "row_weight": row_weight, "col_weight": col_weight, "w_bin": w_bin, "tile_col": tile_col, "w_kernel": w_kernel}


def reference(vis, row_weight, col_weight, w_bin, tile_col, w_kernel):
    total_blocks = CHANS * BLOCKS
    vis_all = vis.reshape(total_blocks // BLK_DEV, BLK_DEV, 2, VIS)
    rows_all = row_weight.reshape(total_blocks // BLK_DEV, BLK_DEV, KROWS, VIS)
    cols_all = col_weight.reshape(total_blocks // BLK_DEV, BLK_DEV, VIS, QW)
    seg_all = (w_bin[:, :, 0] * TC + tile_col).astype(jnp.int32).reshape(total_blocks // BLK_DEV, BLK_DEV)

    def step(acc, group):
        vis_g, rows_g, cols_g, seg_g = group
        weighted = (rows_g.astype(jnp.float32)[:, None, :, :] * vis_g.astype(jnp.float32)[:, :, None, :]).astype(jnp.bfloat16)
        patch = jnp.einsum('ghkv,gvq->gkhq', weighted.astype(jnp.float32), cols_g.astype(jnp.float32))
        patch = patch.reshape(BLK_DEV, KROWS, 2 * QW)
        return acc.at[seg_g].add(patch), None

    start = jnp.zeros((NW * TC, KROWS, 2 * QW), jnp.float32)
    acc, _ = lax.scan(step, start, (vis_all, rows_all, cols_all, seg_all))
    pre_rounded = acc.reshape(NW, TC, KROWS, 2 * QW).astype(jnp.bfloat16)
    return jnp.einsum('wtkq,wqr->wktr', pre_rounded.astype(jnp.float32), w_kernel.astype(jnp.float32))
```

```python
import functools
import jax
import jax.numpy as jnp
from jax import lax
from jax.experimental import pallas as pl
from jax.experimental.pallas import tpu as pltpu
from jax.sharding import PartitionSpec as P

QW = 256
GC = 4096
MESH = pl.DeviceIdType.MESH
LIMIT = 63 * 1024 * 1024
GROUPS = 8
PIECES = 4
NEAR = 0
HOP = 0


def flip(z, k, planes):
    total, bit = 0, 1
    while bit < planes:
        total = total + ((z // bit + k // bit) % 2) * bit
        bit = 2 * bit
    return total


def write_table(table, bins, spots, cells, tiles):
    count = bins.shape[1]
    down = lax.broadcasted_iota(jnp.int32, (count, count), 0)
    along = lax.broadcasted_iota(jnp.int32, (count, count), 1)
    flat = jnp.broadcast_to(bins * tiles + spots, (count, count))
    tall = jnp.max(jnp.where(down == along, flat, 0), axis=1, keepdims=True)
    before = jnp.max(jnp.where((tall == flat) & (down < along), down + 1, 0), axis=0, keepdims=True)
    table[...] = jnp.zeros(table.shape, jnp.int32)
    table[0:1, 0:count] = before
    deep = lax.broadcasted_iota(jnp.int32, (count, 128), 0)
    wide = lax.broadcasted_iota(jnp.int32, (count, 128), 1)
    for r in range(-(-cells // 128)):
        named = tall == wide + r * 128
        table[1 + r:2 + r, :] = jnp.max(jnp.where(named, deep + 1, 0), axis=0, keepdims=True)


def loop(start, stop, step):
    def body(i, carry):
        step(i)
        return carry
    lax.fori_loop(start, stop, body, 0)


def over_planes(start, stop, step):
    if stop - start <= 4:
        for k in range(stop - 1, start - 1, -1):
            step(k)
    else:
        loop(0, stop - start, lambda i: step(stop - 1 - i))


def exchange_kernel(
    planes, tiles, groups, near, hop, bins, spots, vis, rows, cols, kern, out,
    bins_v, spots_v, tab_s, tab_v, vis_v, rows_v, cols_v, kern_v, runs, dout, dgot, xout, xgot, zgot, ngot, hgot,
    lsem, psem, ssend, srecv, dsend, drecv, xsend, xrecv, zsend, zrecv, nsend, nrecv, hsend, hrecv,
):
    me, mine = lax.axis_index("chan"), lax.axis_index("tm")
    core, row = me % 2, me // 2
    pair = {"chan": row * 2 + 1 - core}
    across = {"chan": (1 - row) * 2 + core}
    count, share = rows_v.shape[0], rows_v.shape[3]
    size = tiles // groups
    piece = count // PIECES
    half = xout.dtype

    def plane(k):
        return flip(mine, k, planes)

    small = [
        pltpu.make_async_copy(src, dst, lsem.at[i])
        for i, (src, dst) in enumerate(((bins, bins_v), (spots, spots_v), (vis, vis_v), (kern, kern_v)))
    ]
    parts = []
    for p in range(PIECES):
        cut = pl.ds(p * piece, piece)
        parts.append([
            pltpu.make_async_copy(rows.at[cut], rows_v.at[cut], psem.at[0, p]),
            pltpu.make_async_copy(cols.at[cut], cols_v.at[cut], psem.at[1, p]),
        ])
    for copy in small[:3] + sum(parts, []) + small[3:]:
        copy.start()

    barrier = pltpu.get_barrier_semaphore()
    pl.semaphore_signal(barrier, inc=1, device_id=pair, device_id_type=MESH)
    pl.semaphore_signal(barrier, inc=1, device_id=across, device_id_type=MESH)
    loop(1, planes, lambda k: pl.semaphore_signal(barrier, inc=1, device_id={"tm": plane(k)}, device_id_type=MESH))

    for copy in small[:2]:
        copy.wait()
    write_table(tab_v.at[0], bins_v[...], spots_v[...], planes * tiles, tiles)
    tables = [pltpu.make_async_copy(tab_v.at[i], tab_s.at[i], lsem.at[4 + i]) for i in range(2)]
    tables[0].start()
    swap = pltpu.make_async_remote_copy(
        src_ref=tab_v.at[0], dst_ref=tab_v.at[1], send_sem=ssend, recv_sem=srecv, device_id=pair, device_id_type=MESH,
    )
    for s in range(2):
        runs[s, 0] = jnp.zeros(runs.shape[2:], runs.dtype)

    def entry(s, i):
        return tab_s[s, i // 128, i % 128]

    def d_copy(s, p):
        cut = pl.ds(p * piece, piece)
        return pltpu.make_async_remote_copy(
            src_ref=dout.at[s, cut], dst_ref=dgot.at[s, cut], send_sem=dsend.at[s, p], recv_sem=drecv.at[s, p],
            device_id=pair, device_id_type=MESH,
        )

    def chain(s, b, found):
        last = entry(s, b)
        runs[s, b + 1, :, 0:QW] = found[:share] + runs[s, last, :, 0:QW]
        runs[s, b + 1, :, QW:2 * QW] = found[share:] + runs[s, last, :, QW:2 * QW]

    batch = 2 if piece % 2 == 0 else 1

    def build(s, x, p):
        def step(i):
            found = []
            for u in range(batch):
                b = p * piece + i * batch + u
                own, other = rows_v[b, x, core], rows_v[b, x, 1 - core]
                real, imag = vis_v[b, 0:1, :], vis_v[b, 1:2, :]
                weighted = jnp.concatenate([own * real, own * imag, other * real, other * imag], axis=0)
                found.append(jnp.dot(weighted, cols_v[b], preferred_element_type=jnp.float32))
            for u in range(batch):
                b = p * piece + i * batch + u
                dout[s, b] = found[u][2 * share:].astype(half)
                chain(0, b, found[u][:2 * share])
        loop(0, piece // batch, step)

    def join(s, p):
        def step(i):
            for u in range(batch):
                b = p * piece + i * batch + u
                chain(1, b, dgot[s, b].astype(jnp.float32))
        loop(0, piece // batch, step)

    def cell(w, t):
        i = 128 + w * tiles + t
        return runs[0, entry(0, i)] + runs[1, entry(1, i)]

    def cut_of(g):
        return pl.ds(g * size, size)

    def x_copy(k, g):
        w = plane(k)
        return pltpu.make_async_remote_copy(
            src_ref=xout.at[w, cut_of(g)], dst_ref=xgot.at[w, cut_of(g)],
            send_sem=xsend.at[k, g], recv_sem=xrecv.at[k, g], device_id=across, device_id_type=MESH,
        )

    def z_copy(k, g):
        w = plane(k)
        return pltpu.make_async_remote_copy(
            src_ref=xgot.at[w, cut_of(g)], dst_ref=zgot.at[k - 1, cut_of(g)],
            send_sem=zsend.at[k - 1, g], recv_sem=zrecv.at[k - 1, g], device_id={"tm": w}, device_id_type=MESH,
        )

    small[2].wait()
    tables[0].wait()
    for p in range(PIECES):
        for copy in parts[p]:
            copy.wait()
        build(0, 1 - row, p)
        if p == 0:
            pl.semaphore_wait(barrier, planes + 1)
            swap.start()
        d_copy(0, p).start()
    swap.wait_recv()
    tables[1].start()
    tables[1].wait()
    for p in range(PIECES):
        d_copy(0, p).wait_recv()
        join(0, p)

    def fill(k, g):
        w = plane(k)
        for u in range(size):
            t = g * size + u
            xout[w, t] = cell(w, t).astype(half)

    def send(k, g):
        fill(k, g)
        x_copy(k, g).start()

    over_planes(1, planes, lambda k: loop(0, groups, lambda g: send(k, g)))
    loop(0, groups, lambda g: send(0, g))

    for p in range(PIECES):
        build(1, row, p)
        d_copy(1, p).start()
    for p in range(PIECES):
        d_copy(1, p).wait_recv()
        join(1, p)

    def forward(k, g):
        w = plane(k)
        x_copy(k, g).wait_recv()
        for u in range(size):
            t = g * size + u
            xgot[w, t] = (cell(w, t) + xgot[w, t].astype(jnp.float32)).astype(half)
        z_copy(k, g).start()

    over_planes(1, planes, lambda k: loop(0, groups, lambda g: forward(k, g)))
    small[3].wait()

    def finish(g):
        x_copy(0, g).wait_recv()
        loop(1, planes, lambda k: z_copy(k, g).wait_recv())
        found = []
        for u in range(size):
            t = g * size + u
            total = cell(mine, t) + xgot[mine, t].astype(jnp.float32)

            def add(k, total):
                return total + zgot[k - 1, t].astype(jnp.float32)
            found.append(lax.fori_loop(1, planes, add, total, unroll=planes <= 4).astype(jnp.bfloat16))
        done = jnp.dot(jnp.concatenate(found, axis=0), kern_v[...], preferred_element_type=jnp.float32)
        for u in range(size):
            out[:, g * size + u, :] = done[u * share:(u + 1) * share]

    for g in range(groups):
        finish(g)

    swap.wait_send()
    for s in range(2):
        for p in range(PIECES):
            d_copy(s, p).wait_send()

    def leave(g):
        loop(0, planes, lambda k: x_copy(k, g).wait_send())
        loop(1, planes, lambda k: z_copy(k, g).wait_send())
    loop(0, groups, leave)


def exchange(bins, spots, vis, rows, cols, kern, planes, tiles):
    count, fold, _, share, width = rows.shape
    wide = 2 * cols.shape[2]
    groups = GROUPS
    near, hop = (NEAR, HOP) if planes == 4 else (0, 0)
    size = tiles // groups
    any_spec = pl.BlockSpec(memory_space=pltpu.HBM)
    half = jnp.bfloat16
    dma = pltpu.SemaphoreType.DMA
    table = (-(-(1 + -(-planes * tiles // 128)) // 8) * 8, 128)
    return pl.pallas_call(
        functools.partial(exchange_kernel, planes, tiles, groups, near, hop),
        out_shape=jax.ShapeDtypeStruct((share, tiles, wide), jnp.float32),
        in_specs=[any_spec] * 6,
        out_specs=pl.BlockSpec(memory_space=pltpu.VMEM),
        scratch_shapes=[
            pltpu.VMEM(bins.shape, jnp.int32),
            pltpu.VMEM(spots.shape, jnp.int32),
            pltpu.SMEM((2,) + table, jnp.int32),
            pltpu.VMEM((2,) + table, jnp.int32),
            pltpu.VMEM(vis.shape, vis.dtype),
            pltpu.VMEM(rows.shape, rows.dtype),
            pltpu.VMEM(cols.shape, cols.dtype),
            pltpu.VMEM(kern.shape, kern.dtype),
            pltpu.VMEM((2, count + 1, share, wide), jnp.float32),
            pltpu.VMEM((2, count, 2 * share, wide // 2), half),
            pltpu.VMEM((2, count, 2 * share, wide // 2), half),
            pltpu.VMEM((planes, tiles, share, wide), half),
            pltpu.VMEM((planes, tiles, share, wide), half),
            pltpu.VMEM((planes - 1, tiles, share, wide), half),
            pltpu.VMEM((max(near, 1) * size, share, wide), half),
            pltpu.VMEM((max(hop, 1) * size, share, wide), half),
            dma((6,)),
            dma((2, PIECES)),
            dma,
            dma,
            dma((2, PIECES)),
            dma((2, PIECES)),
            dma((planes, groups)),
            dma((planes, groups)),
            dma((planes - 1, groups)),
            dma((planes - 1, groups)),
            dma((max(near, 1),)),
            dma((max(near, 1),)),
            dma((max(hop, 1),)),
            dma((max(hop, 1),)),
        ],
        compiler_params=pltpu.CompilerParams(
            collective_id=0, has_side_effects=True, vmem_limit_bytes=LIMIT
        ),
        name="exchange",
    )(bins, spots, vis, rows, cols, kern)


def body(vis, row_weight, col_weight, w_bin, tile_col, w_kernel):
    planes = lax.axis_size("tm")
    chans = lax.axis_size("chan")
    count, rows_k, width_v = row_weight.shape[1:]
    tile_count = GC // QW
    fold = chans // 2
    bins = w_bin.reshape(1, count)
    rows = row_weight[0].reshape(count, fold, 2, rows_k // chans, width_v)
    result = exchange(bins, tile_col, vis[0], rows, col_weight[0], w_kernel[0], planes, tile_count)
    return result[None]


def solution(mesh):
    in_specs = (
        P(("groups", "chan"), "tm", None, None),
        P(("groups", "chan"), "tm", None, None),
        P(("groups", "chan"), "tm", None, None),
        P(("groups", "chan"), "tm", None),
        P(("groups", "chan"), "tm"),
        P(("groups", "tm"), None, None),
    )
    out_specs = P(("groups", "tm"), "chan", None, None)
    return jax.shard_map(body, mesh=mesh, in_specs=in_specs, out_specs=out_specs, check_vma=False)
```

```python
import functools
import jax
import jax.numpy as jnp
from jax import lax
from jax.experimental import pallas as pl
from jax.experimental.pallas import tpu as pltpu
from jax.sharding import PartitionSpec as P

QW = 256
GC = 4096
MESH = pl.DeviceIdType.MESH
LIMIT = 63 * 1024 * 1024
GROUPS = 8
PIECES = 4
NEAR = 4
HOP = 4


def flip(z, k, planes):
    total, bit = 0, 1
    while bit < planes:
        total = total + ((z // bit + k // bit) % 2) * bit
        bit = 2 * bit
    return total


def write_table(table, bins, spots, cells, tiles):
    count = bins.shape[1]
    down = lax.broadcasted_iota(jnp.int32, (count, count), 0)
    along = lax.broadcasted_iota(jnp.int32, (count, count), 1)
    flat = jnp.broadcast_to(bins * tiles + spots, (count, count))
    tall = jnp.max(jnp.where(down == along, flat, 0), axis=1, keepdims=True)
    before = jnp.max(jnp.where((tall == flat) & (down < along), down + 1, 0), axis=0, keepdims=True)
    table[...] = jnp.zeros(table.shape, jnp.int32)
    table[0:1, 0:count] = before
    deep = lax.broadcasted_iota(jnp.int32, (count, 128), 0)
    wide = lax.broadcasted_iota(jnp.int32, (count, 128), 1)
    for r in range(-(-cells // 128)):
        named = tall == wide + r * 128
        table[1 + r:2 + r, :] = jnp.max(jnp.where(named, deep + 1, 0), axis=0, keepdims=True)


def loop(start, stop, step):
    def body(i, carry):
        step(i)
        return carry
    lax.fori_loop(start, stop, body, 0)


def over_planes(start, stop, step):
    if stop - start <= 4:
        for k in range(stop - 1, start - 1, -1):
            step(k)
    else:
        loop(0, stop - start, lambda i: step(stop - 1 - i))


def exchange_kernel(
    planes, tiles, groups, near, hop, bins, spots, vis, rows, cols, kern, out,
    bins_v, spots_v, tab_s, tab_v, vis_v, rows_v, cols_v, kern_v, runs, dout, dgot, xout, xgot, zgot, ngot, hgot,
    lsem, psem, ssend, srecv, dsend, drecv, xsend, xrecv, zsend, zrecv, nsend, nrecv, hsend, hrecv,
):
    me, mine = lax.axis_index("chan"), lax.axis_index("tm")
    core, row = me % 2, me // 2
    pair = {"chan": row * 2 + 1 - core}
    across = {"chan": (1 - row) * 2 + core}
    count, share = rows_v.shape[0], rows_v.shape[3]
    size = tiles // groups
    piece = count // PIECES
    half = xout.dtype
    edge = mine % (planes - 1) == 0

    def plane(k):
        return flip(mine, k, planes)

    small = [
        pltpu.make_async_copy(src, dst, lsem.at[i])
        for i, (src, dst) in enumerate(((bins, bins_v), (spots, spots_v), (vis, vis_v), (kern, kern_v)))
    ]
    parts = []
    for p in range(PIECES):
        cut = pl.ds(p * piece, piece)
        parts.append([
            pltpu.make_async_copy(rows.at[cut], rows_v.at[cut], psem.at[0, p]),
            pltpu.make_async_copy(cols.at[cut], cols_v.at[cut], psem.at[1, p]),
        ])
    for copy in small[:3] + sum(parts, []) + small[3:]:
        copy.start()

    barrier = pltpu.get_barrier_semaphore()
    pl.semaphore_signal(barrier, inc=1, device_id=pair, device_id_type=MESH)
    pl.semaphore_signal(barrier, inc=1, device_id=across, device_id_type=MESH)
    loop(1, planes, lambda k: pl.semaphore_signal(barrier, inc=1, device_id={"tm": plane(k)}, device_id_type=MESH))

    tables = [pltpu.make_async_copy(tab_v.at[i], tab_s.at[i], lsem.at[4 + i]) for i in range(2)]
    swap = pltpu.make_async_remote_copy(
        src_ref=tab_v.at[0], dst_ref=tab_v.at[1], send_sem=ssend, recv_sem=srecv, device_id=pair, device_id_type=MESH,
    )
    for s in range(2):
        runs[s, 0] = jnp.zeros(runs.shape[2:], runs.dtype)
    if hop:
        @pl.when(edge)
        def _():
            zgot[planes - 2, pl.ds((groups - hop) * size, hop * size)] = jnp.zeros(hgot.shape, half)
            hgot[...] = jnp.zeros(hgot.shape, half)

    def entry(s, i):
        return tab_s[s, i // 128, i % 128]

    def d_copy(s, p):
        cut = pl.ds(p * piece, piece)
        return pltpu.make_async_remote_copy(
            src_ref=dout.at[s, cut], dst_ref=dgot.at[s, cut], send_sem=dsend.at[s, p], recv_sem=drecv.at[s, p],
            device_id=pair, device_id_type=MESH,
        )

    def build(s, x, p):
        found = []
        for b in range(p * piece, (p + 1) * piece):
            own, other = rows_v[b, x, core], rows_v[b, x, 1 - core]
            real, imag = vis_v[b, 0:1, :], vis_v[b, 1:2, :]
            weighted = jnp.concatenate([own * real, own * imag, other * real, other * imag], axis=0)
            found = jnp.dot(weighted, cols_v[b], preferred_element_type=jnp.float32)
            dout[s, b] = found[2 * share:].astype(half)
            runs[0, b + 1, :, 0:QW] = found[:share]
            runs[0, b + 1, :, QW:2 * QW] = found[share:2 * share]

    batch = 4 if piece % 4 == 0 else 1

    def chain(start, stop):
        def step(i):
            for u in range(batch):
                b = start + i * batch + u
                runs[0, b + 1] = runs[0, b + 1] + runs[0, entry(0, b)]
        loop(0, (stop - start) // batch, step)

    def join(s, p):
        def step(i):
            for u in range(batch):
                b = p * piece + i * batch + u
                found, last = dgot[s, b].astype(jnp.float32), entry(1, b)
                runs[1, b + 1, :, 0:QW] = found[:share] + runs[1, last, :, 0:QW]
                runs[1, b + 1, :, QW:2 * QW] = found[share:] + runs[1, last, :, QW:2 * QW]
        loop(0, piece // batch, step)

    def cell(w, t):
        i = 128 + w * tiles + t
        return runs[0, entry(0, i)] + runs[1, entry(1, i)]

    def cut_of(g):
        return pl.ds(g * size, size)

    def x_copy(k, g):
        w = plane(k)
        return pltpu.make_async_remote_copy(
            src_ref=xout.at[w, cut_of(g)], dst_ref=xgot.at[w, cut_of(g)],
            send_sem=xsend.at[k, g], recv_sem=xrecv.at[k, g], device_id=across, device_id_type=MESH,
        )

    def z_copy(k, g):
        w = plane(k)
        return pltpu.make_async_remote_copy(
            src_ref=xgot.at[w, cut_of(g)], dst_ref=zgot.at[k - 1, cut_of(g)],
            send_sem=zsend.at[k - 1, g], recv_sem=zrecv.at[k - 1, g], device_id={"tm": w}, device_id_type=MESH,
        )

    def near_copy(g):
        cut = pl.ds((g - (groups - near)) * size, size)
        return pltpu.make_async_remote_copy(
            src_ref=xout.at[plane(1), cut_of(g)], dst_ref=ngot.at[cut],
            send_sem=nsend.at[g - (groups - near)], recv_sem=nrecv.at[g - (groups - near)],
            device_id={"tm": plane(1)}, device_id_type=MESH,
        )

    def hop_copy(g):
        cut = pl.ds((g - (groups - hop)) * size, size)
        return pltpu.make_async_remote_copy(
            src_ref=xgot.at[plane(planes - 1), cut_of(g)], dst_ref=hgot.at[cut],
            send_sem=hsend.at[g - (groups - hop)], recv_sem=hrecv.at[g - (groups - hop)],
            device_id={"tm": plane(1)}, device_id_type=MESH,
        )

    small[2].wait()
    for p in range(PIECES):
        with jax.named_scope("load_wait"):
            for copy in parts[p]:
                copy.wait()
        with jax.named_scope("build_far"):
            build(0, 1 - row, p)
        if p == 0:
            with jax.named_scope("write_table"):
                for copy in small[:2]:
                    copy.wait()
                write_table(tab_v.at[0], bins_v[...], spots_v[...], planes * tiles, tiles)
                tables[0].start()
            with jax.named_scope("barrier"):
                pl.semaphore_wait(barrier, planes + 1)
            swap.start()
        d_copy(0, p).start()
    with jax.named_scope("table"):
        swap.wait_recv()
        tables[1].start()
        tables[0].wait()
    with jax.named_scope("chain_far"):
        chain(0, count)
    tables[1].wait()
    for p in range(PIECES):
        with jax.named_scope("pair_wait"):
            d_copy(0, p).wait_recv()
        with jax.named_scope("join_far"):
            join(0, p)

    def fill(k, g):
        w = plane(k)
        for u in range(size):
            t = g * size + u
            xout[w, t] = cell(w, t).astype(half)

    def send(k, g):
        fill(k, g)
        x_copy(k, g).start()

    with jax.named_scope("fill"):
        def send_all(k):
            shift = groups - hop if planes <= 4 and k == planes - 1 else 0
            loop(0, groups, lambda i: send(k, (i + shift) % groups))
            if near and k == planes - 1:
                def approach(g):
                    fill(1, g)
                    near_copy(g).start()
                loop(groups - near, groups, approach)
        over_planes(2, planes, send_all)
        for k in (1, 0):
            loop(0, groups - near, lambda g: send(k, g))
        loop(groups - near, groups, lambda g: fill(0, g))

    for p in range(PIECES):
        with jax.named_scope("build_near"):
            build(1, row, p)
        d_copy(1, p).start()
    with jax.named_scope("chain_near"):
        chain(0, count)
    for p in range(PIECES):
        with jax.named_scope("join_near"):
            d_copy(1, p).wait_recv()
            join(1, p)

    def gather(k, g, crossed=True, hopped=False):
        w = plane(k)
        if crossed:
            x_copy(k, g).wait_recv()
        if hopped:
            pl.when(jnp.logical_not(edge))(lambda: hop_copy(g).wait_recv())
        for u in range(size):
            t = g * size + u
            total = cell(w, t)
            if crossed:
                total = total + xgot[w, t].astype(jnp.float32)
            if hopped:
                total = total + hgot[t - (groups - hop) * size].astype(jnp.float32)
            xgot[w, t] = total.astype(half)

    def forward(k, g, crossed=True, hopped=False):
        gather(k, g, crossed, hopped)
        z_copy(k, g).start()

    def detour(g):
        gather(planes - 1, g)
        pl.when(edge)(lambda: hop_copy(g).start())
        pl.when(jnp.logical_not(edge))(lambda: z_copy(planes - 1, g).start())

    def merge(g):
        near_copy(g).wait_recv()
        for u in range(size):
            t = g * size + u
            arrived = ngot[t - (groups - near) * size].astype(jnp.float32)
            xout[mine, t] = (xout[mine, t].astype(jnp.float32) + arrived).astype(half)
        x_copy(0, g).start()

    def forward_all(k):
        with jax.named_scope("forward"):
            if hop and k == planes - 1:
                loop(groups - hop, groups, detour)
                loop(0, groups - hop, lambda g: forward(k, g))
            elif hop and k == planes - 2:
                loop(0, groups - hop, lambda g: forward(k, g))
                loop(groups - hop, groups, lambda g: forward(k, g, hopped=True))
            else:
                loop(0, groups, lambda g: forward(k, g))
        if near and k == planes - 1:
            with jax.named_scope("merge"):
                loop(groups - near, groups, merge)
    over_planes(2, planes, forward_all)
    with jax.named_scope("forward"):
        loop(0, groups - near, lambda g: forward(1, g))
        loop(groups - near, groups, lambda g: forward(1, g, crossed=False))
    small[3].wait()

    def finish(g):
        with jax.named_scope("finish_x"):
            x_copy(0, g).wait_recv()
        with jax.named_scope("finish_z"):
            loop(1, planes - 1, lambda k: z_copy(k, g).wait_recv())
            if g < groups - hop:
                z_copy(planes - 1, g).wait_recv()
            else:
                pl.when(jnp.logical_not(edge))(lambda: z_copy(planes - 1, g).wait_recv())
        found = []
        for u in range(size):
            t = g * size + u
            total = cell(mine, t) + xgot[mine, t].astype(jnp.float32)

            def add(k, total):
                return total + zgot[k - 1, t].astype(jnp.float32)
            found.append(lax.fori_loop(1, planes, add, total, unroll=planes <= 4).astype(jnp.bfloat16))
        done = jnp.dot(jnp.concatenate(found, axis=0), kern_v[...], preferred_element_type=jnp.float32)
        for u in range(size):
            out[:, g * size + u, :] = done[u * share:(u + 1) * share]

    for g in range(groups):
        with jax.named_scope("finish"):
            finish(g)

    swap.wait_send()
    for s in range(2):
        for p in range(PIECES):
            d_copy(s, p).wait_send()

    def leave(g):
        x_copy(0, g).wait_send()
        loop(2, planes, lambda k: x_copy(k, g).wait_send())
        loop(1, planes - 1, lambda k: z_copy(k, g).wait_send())
    loop(0, groups, leave)
    loop(0, groups - near, lambda g: x_copy(1, g).wait_send())
    loop(groups - near, groups, lambda g: near_copy(g).wait_send())
    loop(0, groups - hop, lambda g: z_copy(planes - 1, g).wait_send())

    def depart(g):
        pl.when(edge)(lambda: hop_copy(g).wait_send())
        pl.when(jnp.logical_not(edge))(lambda: z_copy(planes - 1, g).wait_send())
    loop(groups - hop, groups, depart)


def exchange(bins, spots, vis, rows, cols, kern, planes, tiles):
    count, fold, _, share, width = rows.shape
    wide = 2 * cols.shape[2]
    groups = GROUPS
    near, hop = (NEAR, HOP) if planes == 4 else (0, 0)
    size = tiles // groups
    any_spec = pl.BlockSpec(memory_space=pltpu.HBM)
    half = jnp.bfloat16
    dma = pltpu.SemaphoreType.DMA
    table = (-(-(1 + -(-planes * tiles // 128)) // 8) * 8, 128)
    grids = (2 * planes + planes - 1 + 2) * tiles * share * wide * 2
    held = 2 * (rows.size + cols.size + kern.size) + 8 * (count + 1) * share * wide + 8 * count * share * wide
    limit = min(LIMIT, grids + held + 6 * 1024 * 1024)
    operands = [pltpu.with_memory_space_constraint(a, pltpu.HBM) for a in (bins, spots, vis, rows, cols, kern)]
    return pl.pallas_call(
        functools.partial(exchange_kernel, planes, tiles, groups, near, hop),
        out_shape=jax.ShapeDtypeStruct((share, tiles, wide), jnp.float32),
        in_specs=[any_spec] * 6,
        out_specs=pl.BlockSpec(memory_space=pltpu.VMEM),
        scratch_shapes=[
            pltpu.VMEM(bins.shape, jnp.int32),
            pltpu.VMEM(spots.shape, jnp.int32),
            pltpu.SMEM((2,) + table, jnp.int32),
            pltpu.VMEM((2,) + table, jnp.int32),
            pltpu.VMEM(vis.shape, vis.dtype),
            pltpu.VMEM(rows.shape, rows.dtype),
            pltpu.VMEM(cols.shape, cols.dtype),
            pltpu.VMEM(kern.shape, kern.dtype),
            pltpu.VMEM((2, count + 1, share, wide), jnp.float32),
            pltpu.VMEM((2, count, 2 * share, wide // 2), half),
            pltpu.VMEM((2, count, 2 * share, wide // 2), half),
            pltpu.VMEM((planes, tiles, share, wide), half),
            pltpu.VMEM((planes, tiles, share, wide), half),
            pltpu.VMEM((planes - 1, tiles, share, wide), half),
            pltpu.VMEM((max(near, 1) * size, share, wide), half),
            pltpu.VMEM((max(hop, 1) * size, share, wide), half),
            dma((6,)),
            dma((2, PIECES)),
            dma,
            dma,
            dma((2, PIECES)),
            dma((2, PIECES)),
            dma((planes, groups)),
            dma((planes, groups)),
            dma((planes - 1, groups)),
            dma((planes - 1, groups)),
            dma((max(near, 1),)),
            dma((max(near, 1),)),
            dma((max(hop, 1),)),
            dma((max(hop, 1),)),
        ],
        compiler_params=pltpu.CompilerParams(
            collective_id=0, has_side_effects=True, vmem_limit_bytes=limit
        ),
        name="exchange",
    )(*operands)


def body(vis, row_weight, col_weight, w_bin, tile_col, w_kernel):
    planes = lax.axis_size("tm")
    chans = lax.axis_size("chan")
    count, rows_k, width_v = row_weight.shape[1:]
    tile_count = GC // QW
    fold = chans // 2
    bins = w_bin.reshape(1, count)
    rows = row_weight[0].reshape(count, fold, 2, rows_k // chans, width_v)
    result = exchange(bins, tile_col, vis[0], rows, col_weight[0], w_kernel[0], planes, tile_count)
    return result[None]


def solution(mesh):
    in_specs = (
        P(("groups", "chan"), "tm", None, None),
        P(("groups", "chan"), "tm", None, None),
        P(("groups", "chan"), "tm", None, None),
        P(("groups", "chan"), "tm", None),
        P(("groups", "chan"), "tm"),
        P(("groups", "tm"), None, None),
    )
    out_specs = P(("groups", "tm"), "chan", None, None)
    return jax.shard_map(body, mesh=mesh, in_specs=in_specs, out_specs=out_specs, check_vma=False)
```

```python
import functools
import jax
import jax.numpy as jnp
from jax import lax
from jax.experimental import pallas as pl
from jax.experimental.pallas import tpu as pltpu
from jax.sharding import PartitionSpec as P

QW = 256
GC = 4096
MESH = pl.DeviceIdType.MESH
LIMIT = 63 * 1024 * 1024
PARTS = 4
TURNS = 8
PIECES = 4
NEAR = 2


def write_table(table, bins, spots, cells, tiles):
    count = bins.shape[1]
    down = lax.broadcasted_iota(jnp.int32, (count, count), 0)
    along = lax.broadcasted_iota(jnp.int32, (count, count), 1)
    flat = jnp.broadcast_to(bins * tiles + spots, (count, count))
    tall = jnp.max(jnp.where(down == along, flat, 0), axis=1, keepdims=True)
    before = jnp.max(jnp.where((tall == flat) & (down < along), down + 1, 0), axis=0, keepdims=True)
    table[...] = jnp.zeros(table.shape, jnp.int32)
    table[0:1, 0:count] = before
    deep = lax.broadcasted_iota(jnp.int32, (count, 128), 0)
    wide = lax.broadcasted_iota(jnp.int32, (count, 128), 1)
    for r in range(-(-cells // 128)):
        named = tall == wide + r * 128
        table[1 + r:2 + r, :] = jnp.max(jnp.where(named, deep + 1, 0), axis=0, keepdims=True)


def loop(start, stop, step):
    def body(i, carry):
        step(i)
        return carry
    lax.fori_loop(start, stop, body, 0)


def over_planes(start, stop, step):
    if stop - start <= 4:
        for k in range(start, stop):
            step(k)
    else:
        loop(start, stop, step)


def exchange_kernel(
    planes, tiles, groups, turns, near, bins, spots, vis, rows, cols, kern, out,
    bins_v, spots_v, tab_s, tab_v, vis_v, rows_v, cols_v, kern_v, runs, dout, dgot, xout, xgot, zgot, ngot,
    lsem, psem, ssend, srecv, dsend, drecv, xsend, xrecv, yrecv, zsend, zrecv, nrecv,
):
    me, mine = lax.axis_index("chan"), lax.axis_index("tm")
    core, row = me % 2, me // 2
    pair = {"chan": row * 2 + 1 - core}
    across = {"chan": (1 - row) * 2 + core}
    count, share = rows_v.shape[0], rows_v.shape[3]
    size, step = tiles // groups, tiles // turns
    piece = count // PIECES
    half = xout.dtype
    edge = mine % (planes - 1) == 0

    up = mine // (planes // 2)
    reach = up * mine + (1 - up) * (planes - 1 - mine)
    beside = {"tm": mine + 1 - 2 * (mine % 2)}

    def less(a, b):
        return (planes - 1 + b - a) // planes

    def plane(i):
        late = i // reach
        v = (1 - late) * i + late * (planes - 1 - (i - reach))
        return up * v + (1 - up) * (planes - 1 - v)

    def slot(w):
        return w + less(w, mine) * (1 - less(w, mine - 1)) * (planes - w)

    small = [
        pltpu.make_async_copy(src, dst, lsem.at[i])
        for i, (src, dst) in enumerate(((bins, bins_v), (spots, spots_v), (vis, vis_v), (kern, kern_v)))
    ]
    parts = []
    for p in range(PIECES):
        cut = pl.ds(p * piece, piece)
        parts.append([
            pltpu.make_async_copy(rows.at[cut], rows_v.at[cut], psem.at[0, p]),
            pltpu.make_async_copy(cols.at[cut], cols_v.at[cut], psem.at[1, p]),
        ])
    for copy in small[:3] + sum(parts, []) + small[3:]:
        copy.start()

    barrier = pltpu.get_barrier_semaphore()
    pl.semaphore_signal(barrier, inc=1, device_id=pair, device_id_type=MESH)
    pl.semaphore_signal(barrier, inc=1, device_id=across, device_id_type=MESH)

    def greet(step):
        pl.semaphore_signal(barrier, inc=1, device_id={"tm": mine + step}, device_id_type=MESH)
    pl.when(mine > 0)(lambda: greet(-1))
    pl.when(mine < planes - 1)(lambda: greet(1))

    tables = [pltpu.make_async_copy(tab_v.at[i], tab_s.at[i], lsem.at[4 + i]) for i in range(2)]
    swap = pltpu.make_async_remote_copy(
        src_ref=tab_v.at[0], dst_ref=tab_v.at[1], send_sem=ssend, recv_sem=srecv, device_id=pair, device_id_type=MESH,
    )
    for s in range(2):
        runs[s, 0] = jnp.zeros(runs.shape[2:], runs.dtype)

    @pl.when(edge)
    def _():
        zgot[(mine // (planes - 1)) * planes] = jnp.zeros(zgot.shape[1:], half)

    def entry(s, i):
        return tab_s[s, i // 128, i % 128]

    def d_copy(s, p):
        cut = pl.ds(p * piece, piece)
        return pltpu.make_async_remote_copy(
            src_ref=dout.at[s, cut], dst_ref=dgot.at[s, cut], send_sem=dsend, recv_sem=drecv.at[s, p],
            device_id=pair, device_id_type=MESH,
        )

    def build(s, x, p):
        found = []
        for b in range(p * piece, (p + 1) * piece):
            own, other = rows_v[b, x, core], rows_v[b, x, 1 - core]
            real, imag = vis_v[b, 0:1, :], vis_v[b, 1:2, :]
            weighted = jnp.concatenate([own * real, own * imag, other * real, other * imag], axis=0)
            found = jnp.dot(weighted, cols_v[b], preferred_element_type=jnp.float32)
            dout[s, b] = found[2 * share:].astype(half)
            runs[0, b + 1, :, 0:QW] = found[:share]
            runs[0, b + 1, :, QW:2 * QW] = found[share:2 * share]

    batch = 4 if piece % 4 == 0 else 1

    def chain(start, stop):
        def step(i):
            for u in range(batch):
                b = start + i * batch + u
                runs[0, b + 1] = runs[0, b + 1] + runs[0, entry(0, b)]
        loop(0, (stop - start) // batch, step)

    def join(s, p):
        def step(i):
            for u in range(batch):
                b = p * piece + i * batch + u
                found, last = dgot[s, b].astype(jnp.float32), entry(1, b)
                runs[1, b + 1, :, 0:QW] = found[:share] + runs[1, last, :, 0:QW]
                runs[1, b + 1, :, QW:2 * QW] = found[share:] + runs[1, last, :, QW:2 * QW]
        loop(0, piece // batch, step)

    def cell(w, t):
        i = 128 + w * tiles + t
        return runs[0, entry(0, i)] + runs[1, entry(1, i)]

    later = turns - near * turns // groups

    def cut_of(g):
        return pl.ds(g * size, size)

    def x_copy(i, g):
        w = plane(i)
        return pltpu.make_async_remote_copy(
            src_ref=xout.at[w, cut_of(g)], dst_ref=xgot.at[w, cut_of(g)],
            send_sem=xsend, recv_sem=xrecv.at[i, g], device_id=across, device_id_type=MESH,
        )

    def y_copy(j):
        cut = pl.ds(j * step, step)
        return pltpu.make_async_remote_copy(
            src_ref=xout.at[mine, cut], dst_ref=xgot.at[mine, cut],
            send_sem=xsend, recv_sem=yrecv.at[j], device_id=across, device_id_type=MESH,
        )

    def z_copy(w, g):
        return pltpu.make_async_remote_copy(
            src_ref=xgot.at[w, cut_of(g)], dst_ref=zgot.at[slot(w), cut_of(g)],
            send_sem=zsend, recv_sem=zrecv.at[slot(w), g],
            device_id={"tm": mine + 2 * less(mine, w) - 1}, device_id_type=MESH,
        )

    def z_wait(at, g):
        pltpu.make_async_remote_copy(
            src_ref=xgot.at[0, cut_of(g)], dst_ref=zgot.at[at, cut_of(g)],
            send_sem=zsend, recv_sem=zrecv.at[at, g], device_id=beside, device_id_type=MESH,
        ).wait_recv()

    def near_copy(g):
        at = g - (groups - near)
        return pltpu.make_async_remote_copy(
            src_ref=xout.at[plane(planes - 2), cut_of(g)], dst_ref=ngot.at[pl.ds(at * size, size)],
            send_sem=xsend, recv_sem=nrecv.at[at], device_id=beside, device_id_type=MESH,
        )

    small[2].wait()
    for p in range(PIECES):
        with jax.named_scope("load_wait"):
            for copy in parts[p]:
                copy.wait()
        with jax.named_scope("build_far"):
            build(0, 1 - row, p)
        if p == 0:
            with jax.named_scope("write_table"):
                for copy in small[:2]:
                    copy.wait()
                write_table(tab_v.at[0], bins_v[...], spots_v[...], planes * tiles, tiles)
                tables[0].start()
            with jax.named_scope("barrier"):
                pl.semaphore_wait(barrier, 3 + less(0, mine) * less(mine, planes - 1))
            swap.start()
        d_copy(0, p).start()
    with jax.named_scope("table"):
        swap.wait_recv()
        tables[1].start()
        tables[0].wait()
    with jax.named_scope("chain_far"):
        chain(0, count)
    tables[1].wait()
    for p in range(PIECES):
        with jax.named_scope("pair_wait"):
            d_copy(0, p).wait_recv()
        with jax.named_scope("join_far"):
            join(0, p)

    def fill(w, start, many):
        for u in range(many):
            xout[w, start + u] = cell(w, start + u).astype(half)

    def send(i, g):
        fill(plane(i), g * size, size)
        x_copy(i, g).start()

    def send_own(j):
        fill(mine, j * step, step)
        y_copy(j).start()

    def approach(g):
        fill(plane(planes - 2), g * size, size)
        near_copy(g).start()

    with jax.named_scope("fill"):
        loop(0, groups, lambda g: send(0, g))
        loop(groups - near, groups, approach)
        over_planes(1, planes - 2, lambda i: loop(0, groups, lambda g: send(i, g)))
        loop(0, groups - near, lambda g: send(planes - 2, g))
        loop(0, later, send_own)
        loop(later, turns, lambda j: fill(mine, j * step, step))

    for p in range(PIECES):
        with jax.named_scope("build_near"):
            build(1, row, p)
        d_copy(1, p).start()
    with jax.named_scope("chain_near"):
        chain(0, count)
    for p in range(PIECES):
        with jax.named_scope("join_near"):
            d_copy(1, p).wait_recv()
            join(1, p)

    def gather(w, g, crossed, joined):
        for u in range(size):
            t = g * size + u
            total = cell(w, t)
            if crossed:
                total = total + xgot[w, t].astype(jnp.float32)
            if joined:
                total = total + zgot[w, t].astype(jnp.float32)
            xgot[w, t] = total.astype(half)

    def forward(i, g, joined, crossed=True):
        w = plane(i)
        if crossed:
            x_copy(i, g).wait_recv()
        if joined:
            z_wait(w, g)
        gather(w, g, crossed, joined)
        z_copy(w, g).start()

    def merge(g):
        near_copy(g).wait_recv()
        for u in range(size):
            t = g * size + u
            arrived = ngot[t - (groups - near) * size].astype(jnp.float32)
            xout[mine, t] = (xout[mine, t].astype(jnp.float32) + arrived).astype(half)
        for u in range(turns // groups):
            y_copy(g * (turns // groups) + u).start()

    @pl.when(edge)
    def _():
        with jax.named_scope("edge_first"):
            loop(0, groups, lambda g: forward(0, g, False))
            loop(groups - near, groups, merge)
        with jax.named_scope("edge_middle"):
            over_planes(1, planes - 2, lambda i: loop(0, groups, lambda g: forward(i, g, False)))
        with jax.named_scope("edge_last"):
            loop(0, groups - near, lambda g: forward(planes - 2, g, False))
            loop(groups - near, groups, lambda g: forward(planes - 2, g, False, crossed=False))

    @pl.when(jnp.logical_not(edge))
    def _():
        with jax.named_scope("inner_first"):
            loop(0, groups, lambda g: forward(0, g, True))
            loop(groups - near, groups, merge)

        def both(g):
            forward(planes - 3, g, True)
            forward(planes - 2, g + groups - near, True, crossed=False)

        def rest(g):
            forward(planes - 3, g, True)
            forward(planes - 2, g - near, True)
        with jax.named_scope("inner_middle"):
            over_planes(1, planes - 3, lambda i: loop(0, groups, lambda g: forward(i, g, True)))
        with jax.named_scope("inner_both"):
            loop(0, near, both)
            loop(near, groups, rest)

    small[3].wait()

    def finish(j):
        with jax.named_scope("finish_x"):
            y_copy(j).wait_recv()
        if j % (turns // groups) == 0:
            g = j // (turns // groups)
            with jax.named_scope("finish_z"):
                pl.when(mine > 0)(lambda: z_wait(mine, g))
                pl.when(mine < planes - 1)(lambda: z_wait(planes, g))
        found = []
        for u in range(step):
            t = j * step + u
            total = cell(mine, t) + xgot[mine, t].astype(jnp.float32)
            total = total + zgot[mine, t].astype(jnp.float32) + zgot[planes, t].astype(jnp.float32)
            found.append(total.astype(jnp.bfloat16))
        done = jnp.dot(jnp.concatenate(found, axis=0), kern_v[...], preferred_element_type=jnp.float32)
        for u in range(step):
            out[:, j * step + u, :] = done[u * share:(u + 1) * share]

    with jax.named_scope("leave"):
        swap.wait_send()
        pltpu.make_async_remote_copy(
            src_ref=dout, dst_ref=dgot, send_sem=dsend, recv_sem=srecv, device_id=pair, device_id_type=MESH,
        ).wait_send()

    for j in range(turns):
        with jax.named_scope("finish"):
            finish(j)
    with jax.named_scope("leave"):
        pltpu.make_async_remote_copy(
            src_ref=xout, dst_ref=xgot, send_sem=xsend, recv_sem=srecv, device_id=across, device_id_type=MESH,
        ).wait_send()
        pltpu.make_async_remote_copy(
            src_ref=xgot.at[0:planes - 1], dst_ref=zgot.at[0:planes - 1], send_sem=zsend, recv_sem=srecv,
            device_id=beside, device_id_type=MESH,
        ).wait_send()


def exchange(bins, spots, vis, rows, cols, kern, planes, tiles):
    count, fold, _, share, width = rows.shape
    wide = 2 * cols.shape[2]
    groups, turns = PARTS, TURNS
    near = NEAR if planes <= 4 else 0
    size = tiles // groups
    any_spec = pl.BlockSpec(memory_space=pltpu.HBM)
    half = jnp.bfloat16
    dma = pltpu.SemaphoreType.DMA
    table = (-(-(1 + -(-planes * tiles // 128)) // 8) * 8, 128)
    grids = (2 * planes + planes + 1 + 2) * tiles * share * wide * 2
    held = 2 * (rows.size + cols.size + kern.size) + 8 * (count + 1) * share * wide + 8 * count * share * wide
    limit = min(LIMIT, grids + held + 6 * 1024 * 1024)
    operands = [pltpu.with_memory_space_constraint(a, pltpu.HBM) for a in (bins, spots, vis, rows, cols, kern)]
    return pl.pallas_call(
        functools.partial(exchange_kernel, planes, tiles, groups, turns, near),
        out_shape=jax.ShapeDtypeStruct((share, tiles, wide), jnp.float32),
        in_specs=[any_spec] * 6,
        out_specs=pl.BlockSpec(memory_space=pltpu.VMEM),
        scratch_shapes=[
            pltpu.VMEM(bins.shape, jnp.int32),
            pltpu.VMEM(spots.shape, jnp.int32),
            pltpu.SMEM((2,) + table, jnp.int32),
            pltpu.VMEM((2,) + table, jnp.int32),
            pltpu.VMEM(vis.shape, vis.dtype),
            pltpu.VMEM(rows.shape, rows.dtype),
            pltpu.VMEM(cols.shape, cols.dtype),
            pltpu.VMEM(kern.shape, kern.dtype),
            pltpu.VMEM((2, count + 1, share, wide), jnp.float32),
            pltpu.VMEM((2, count, 2 * share, wide // 2), half),
            pltpu.VMEM((2, count, 2 * share, wide // 2), half),
            pltpu.VMEM((planes, tiles, share, wide), half),
            pltpu.VMEM((planes, tiles, share, wide), half),
            pltpu.VMEM((planes + 1, tiles, share, wide), half),
            pltpu.VMEM((max(near, 1) * size, share, wide), half),
            dma((6,)),
            dma((2, PIECES)),
            dma,
            dma,
            dma,
            dma((2, PIECES)),
            dma,
            dma((planes - 1, groups)),
            dma((turns,)),
            dma,
            dma((planes + 1, groups)),
            dma((max(near, 1),)),
        ],
        compiler_params=pltpu.CompilerParams(
            collective_id=0, has_side_effects=True, vmem_limit_bytes=limit
        ),
        name="exchange",
    )(*operands)


def body(vis, row_weight, col_weight, w_bin, tile_col, w_kernel):
    planes = lax.axis_size("tm")
    chans = lax.axis_size("chan")
    count, rows_k, width_v = row_weight.shape[1:]
    tile_count = GC // QW
    fold = chans // 2
    bins = w_bin.reshape(1, count)
    rows = row_weight[0].reshape(count, fold, 2, rows_k // chans, width_v)
    result = exchange(bins, tile_col, vis[0], rows, col_weight[0], w_kernel[0], planes, tile_count)
    return result[None]


def solution(mesh):
    in_specs = (
        P(("groups", "chan"), "tm", None, None),
        P(("groups", "chan"), "tm", None, None),
        P(("groups", "chan"), "tm", None, None),
        P(("groups", "chan"), "tm", None),
        P(("groups", "chan"), "tm"),
        P(("groups", "tm"), None, None),
    )
    out_specs = P(("groups", "tm"), "chan", None, None)
    return jax.shard_map(body, mesh=mesh, in_specs=in_specs, out_specs=out_specs, check_vma=False)
```

```python
import functools
import jax
import jax.numpy as jnp
from jax import lax
from jax.experimental import pallas as pl
from jax.experimental.pallas import tpu as pltpu
from jax.sharding import PartitionSpec as P

QW = 256
GC = 4096
MESH = pl.DeviceIdType.MESH
LIMIT = 63 * 1024 * 1024
PIECES = 4
NEAR = 9


def write_table(table, bins, spots, cells, tiles):
    count = bins.shape[1]
    down = lax.broadcasted_iota(jnp.int32, (count, count), 0)
    along = lax.broadcasted_iota(jnp.int32, (count, count), 1)
    flat = jnp.broadcast_to(bins * tiles + spots, (count, count))
    tall = jnp.max(jnp.where(down == along, flat, 0), axis=1, keepdims=True)
    before = jnp.max(jnp.where((tall == flat) & (down < along), down + 1, 0), axis=0, keepdims=True)
    table[...] = jnp.zeros(table.shape, jnp.int32)
    table[0:1, 0:count] = before
    deep = lax.broadcasted_iota(jnp.int32, (count, 128), 0)
    wide = lax.broadcasted_iota(jnp.int32, (count, 128), 1)
    for r in range(-(-cells // 128)):
        named = tall == wide + r * 128
        table[1 + r:2 + r, :] = jnp.max(jnp.where(named, deep + 1, 0), axis=0, keepdims=True)


def loop(start, stop, step):
    def body(i, carry):
        step(i)
        return carry
    lax.fori_loop(start, stop, body, 0)


def messages(planes, tiles, share):
    quarter, half = tiles // 4, share // 2
    even = [(q * quarter, quarter, 0, share) for q in range(4)]
    if planes != 4:
        own = [(t, 2) for t in range(0, tiles, 2)]
        return [even] * (planes - 1), [], own, tiles
    split = tiles - NEAR
    first = [(t, tiles // 2, r, half) for r in (0, half) for t in (tiles // 2, 0)]
    last = [(0, quarter, 0, share), (quarter, split - quarter, 0, share)]
    middle = split + (NEAR + 1) // 2
    last += [(split, middle - split, 0, share), (middle, tiles - middle, 0, share)]
    near = [(split, NEAR, r, half) for r in (0, half)]
    own = [(t, min(2, split - t)) for t in range(0, split, 2)]
    own += [(t, min(2, tiles - t)) for t in range(split, tiles, 2)]
    return [first, even, last], near, own, split


def exchange_kernel(
    planes, tiles, bins, spots, vis, rows, cols, kern, out,
    bins_v, spots_v, tab_s, tab_v, vis_v, rows_v, cols_v, kern_v, runs, dout, dgot, xout, xgot, zgot, ngot,
    lsem, psem, ssend, srecv, dsend, drecv, xsend, xrecv, yrecv, zsend, zrecv, nrecv,
):
    me, mine = lax.axis_index("chan"), lax.axis_index("tm")
    core, row = me % 2, me // 2
    pair = {"chan": row * 2 + 1 - core}
    across = {"chan": (1 - row) * 2 + core}
    count, share = rows_v.shape[0], rows_v.shape[3]
    half_rows = share // 2
    piece = count // PIECES
    narrow = xout.dtype
    edge = mine % (planes - 1) == 0
    up = mine // (planes // 2)
    reach = up * mine + (1 - up) * (planes - 1 - mine)
    beside = {"tm": mine + 1 - 2 * (mine % 2)}
    lists, near, own_list, split = messages(planes, tiles, share)
    short = len(near) > 0

    def less(a, b):
        return (planes - 1 + b - a) // planes

    def plane(i):
        late = i // reach
        v = (1 - late) * i + late * (planes - 1 - (i - reach))
        return up * v + (1 - up) * (planes - 1 - v)

    def slot(w):
        return w + less(w, mine) * (1 - less(w, mine - 1)) * (planes - w)

    def list_of(i):
        return lists[i] if short else lists[0]

    small = [
        pltpu.make_async_copy(src, dst, lsem.at[i])
        for i, (src, dst) in enumerate(((bins, bins_v), (spots, spots_v), (vis, vis_v), (kern, kern_v)))
    ]
    parts = []
    for p in range(PIECES):
        cut = pl.ds(p * piece, piece)
        parts.append([
            pltpu.make_async_copy(rows.at[cut], rows_v.at[cut], psem.at[0, p]),
            pltpu.make_async_copy(cols.at[cut], cols_v.at[cut], psem.at[1, p]),
        ])
    for copy in small[:3] + sum(parts, []) + small[3:]:
        copy.start()

    barrier = pltpu.get_barrier_semaphore()
    pl.semaphore_signal(barrier, inc=1, device_id=pair, device_id_type=MESH)
    pl.semaphore_signal(barrier, inc=1, device_id=across, device_id_type=MESH)

    def greet(step):
        pl.semaphore_signal(barrier, inc=1, device_id={"tm": mine + step}, device_id_type=MESH)
    pl.when(mine > 0)(lambda: greet(-1))
    pl.when(mine < planes - 1)(lambda: greet(1))

    tables = [pltpu.make_async_copy(tab_v.at[i], tab_s.at[i], lsem.at[4 + i]) for i in range(2)]
    swap = pltpu.make_async_remote_copy(
        src_ref=tab_v.at[0], dst_ref=tab_v.at[1], send_sem=ssend, recv_sem=srecv, device_id=pair, device_id_type=MESH,
    )
    for s in range(2):
        runs[s, 0] = jnp.zeros(runs.shape[2:], runs.dtype)

    @pl.when(edge)
    def _():
        zgot[(mine // (planes - 1)) * planes] = jnp.zeros(zgot.shape[1:], narrow)

    def entry(s, i):
        return tab_s[s, i // 128, i % 128]

    def d_copy(r, p):
        cut = pl.ds(p * (count // 2), count // 2)
        return pltpu.make_async_remote_copy(
            src_ref=dout.at[0, r, cut], dst_ref=dgot.at[0, r, cut], send_sem=dsend, recv_sem=drecv.at[2 * r + p],
            device_id=pair, device_id_type=MESH,
        )

    def e_copy(p):
        cut = pl.ds(p * (count // 2), count // 2)
        return pltpu.make_async_remote_copy(
            src_ref=dout.at[1, :, cut], dst_ref=dgot.at[1, :, cut], send_sem=dsend, recv_sem=drecv.at[4 + p],
            device_id=pair, device_id_type=MESH,
        )

    def build_other(s, x, p):
        for b in range(p * piece, (p + 1) * piece):
            other = rows_v[b, x, 1 - core]
            real, imag = vis_v[b, 0:1, :], vis_v[b, 1:2, :]
            upper, lower = other[:half_rows], other[half_rows:]
            weighted = jnp.concatenate([upper * real, upper * imag, lower * real, lower * imag], axis=0)
            found = jnp.dot(weighted, cols_v[b], preferred_element_type=jnp.float32).astype(narrow)
            dout[s, 0, b] = found[:share]
            dout[s, 1, b] = found[share:]

    def build_own(x, p):
        for b in range(p * piece, (p + 1) * piece):
            own = rows_v[b, x, core]
            real, imag = vis_v[b, 0:1, :], vis_v[b, 1:2, :]
            weighted = jnp.concatenate([own * real, own * imag], axis=0)
            found = jnp.dot(weighted, cols_v[b], preferred_element_type=jnp.float32)
            runs[0, b + 1, :, 0:QW] = found[:share]
            runs[0, b + 1, :, QW:2 * QW] = found[share:]

    batch = 4 if count % 8 == 0 else 1

    def chain(low, high):
        def step(i):
            for u in range(batch):
                b = i * batch + u
                runs[0, b + 1, low:high] = runs[0, b + 1, low:high] + runs[0, entry(0, b), low:high]
        loop(0, count // batch, step)

    def join(s, r, p):
        low, high = r * half_rows, (r + 1) * half_rows

        def step(i):
            for u in range(batch):
                b = p * (count // 2) + i * batch + u
                found, last = dgot[s, r, b].astype(jnp.float32), entry(1, b)
                runs[1, b + 1, low:high, 0:QW] = found[:half_rows] + runs[1, last, low:high, 0:QW]
                runs[1, b + 1, low:high, QW:2 * QW] = found[half_rows:] + runs[1, last, low:high, QW:2 * QW]
        loop(0, count // 2 // batch, step)

    def cell(w, t, low, high):
        i = 128 + w * tiles + t
        return runs[0, entry(0, i), low:high] + runs[1, entry(1, i), low:high]

    def window(ref, w, m):
        start, many, low, deep = m
        return ref.at[w, start:start + many, low:low + deep]

    def x_copy(i, n):
        w, m = plane(i), list_of(i)[n]
        return pltpu.make_async_remote_copy(
            src_ref=window(xout, w, m), dst_ref=window(xgot, w, m),
            send_sem=xsend, recv_sem=xrecv.at[i, n], device_id=across, device_id_type=MESH,
        )

    def y_copy(n):
        m = own_list[n] + (0, share)
        return pltpu.make_async_remote_copy(
            src_ref=window(xout, mine, m), dst_ref=window(xgot, mine, m),
            send_sem=xsend, recv_sem=yrecv.at[n], device_id=across, device_id_type=MESH,
        )

    def z_copy(i, n):
        w, m = plane(i), list_of(i)[n]
        return pltpu.make_async_remote_copy(
            src_ref=window(xgot, w, m), dst_ref=window(zgot, slot(w), m),
            send_sem=zsend, recv_sem=zrecv.at[slot(w), n],
            device_id={"tm": mine + 2 * less(mine, w) - 1}, device_id_type=MESH,
        )

    def z_wait(at, m, n):
        pltpu.make_async_remote_copy(
            src_ref=window(xgot, 0, m), dst_ref=window(zgot, at, m),
            send_sem=zsend, recv_sem=zrecv.at[at, n], device_id=beside, device_id_type=MESH,
        ).wait_recv()

    def near_copy(n):
        start, many, low, deep = near[n]
        return pltpu.make_async_remote_copy(
            src_ref=window(xout, plane(planes - 2), near[n]), dst_ref=ngot.at[:, low:low + deep],
            send_sem=xsend, recv_sem=nrecv.at[n], device_id=beside, device_id_type=MESH,
        )

    def over_tiles(start, many, step):
        pairs = many // 2

        def two(i):
            step(start + 2 * i)
            step(start + 2 * i + 1)
        loop(0, pairs, two)
        if many % 2:
            step(start + many - 1)

    def fill(w, m):
        start, many, low, deep = m

        def step(t):
            xout[w, t, low:low + deep] = cell(w, t, low, low + deep).astype(narrow)
        over_tiles(start, many, step)

    def send(i, n):
        fill(plane(i), list_of(i)[n])
        x_copy(i, n).start()

    def approach(n):
        fill(plane(planes - 2), near[n])
        near_copy(n).start()

    with jax.named_scope("table"):
        for copy in small[:2]:
            copy.wait()
        write_table(tab_v.at[0], bins_v[...], spots_v[...], planes * tiles, tiles)
        tables[0].start()
    with jax.named_scope("vis_wait"):
        small[2].wait()
    for p in range(PIECES):
        with jax.named_scope("load_wait"):
            for copy in parts[p]:
                copy.wait()
        with jax.named_scope("build_other"):
            build_other(0, 1 - row, p)
        if p == PIECES // 2 - 1:
            with jax.named_scope("barrier"):
                pl.semaphore_wait(barrier, 3 + less(0, mine) * less(mine, planes - 1))
            swap.start()
            d_copy(0, 0).start()
    d_copy(0, 1).start()
    d_copy(1, 0).start()
    d_copy(1, 1).start()
    for p in range(PIECES):
        with jax.named_scope("build_own"):
            build_own(1 - row, p)
    with jax.named_scope("swap_wait"):
        swap.wait_recv()
        tables[1].start()
        tables[0].wait()
    with jax.named_scope("chain_far"):
        chain(0, half_rows)
        chain(half_rows, share)
    with jax.named_scope("table_wait"):
        tables[1].wait()
    for p in range(2):
        with jax.named_scope("pair_wait"):
            d_copy(0, p).wait_recv()
        with jax.named_scope("join_far"):
            join(0, 0, p)
    if short:
        with jax.named_scope("fill_first"):
            send(0, 0)
            approach(0)
            send(0, 1)
    for p in range(2):
        with jax.named_scope("pair_wait"):
            d_copy(1, p).wait_recv()
        with jax.named_scope("join_far"):
            join(0, 1, p)
    with jax.named_scope("fill"):
        if short:
            send(0, 2)
            send(0, 3)
            approach(1)
            for n in range(len(lists[1])):
                send(1, n)
            for n in range(2):
                send(2, n)
        else:
            def send_all(i):
                for n in range(len(list_of(i))):
                    send(i, n)
            loop(0, planes - 1, send_all)
        for n, m in enumerate(own_list):
            fill(mine, m + (0, share))
            if m[0] < split:
                y_copy(n).start()

    for p in range(PIECES):
        with jax.named_scope("build_near"):
            build_other(1, row, p)
        if p % 2:
            e_copy(p // (PIECES // 2)).start()
    for p in range(PIECES):
        with jax.named_scope("build_near"):
            build_own(row, p)
    with jax.named_scope("chain_near"):
        chain(0, share)
    for p in range(2):
        with jax.named_scope("join_near"):
            e_copy(p).wait_recv()
            join(1, 0, p)
            join(1, 1, p)

    def gather(w, m, crossed, joined):
        start, many, low, deep = m
        high = low + deep

        def step(t):
            total = cell(w, t, low, high)
            if crossed:
                total = total + xgot[w, t, low:high].astype(jnp.float32)
            if joined:
                total = total + zgot[w, t, low:high].astype(jnp.float32)
            xgot[w, t, low:high] = total.astype(narrow)
        over_tiles(start, many, step)

    def forward(i, n, joined, crossed=True, wait=True):
        w, m = plane(i), list_of(i)[n]
        if crossed:
            x_copy(i, n).wait_recv()
        if joined and wait:
            z_wait(w, m, n)
        gather(w, m, crossed, joined)
        z_copy(i, n).start()

    def merge():
        for n in range(len(near)):
            near_copy(n).wait_recv()

        def step(t):
            arrived = ngot[t - split].astype(jnp.float32)
            xout[mine, t] = (xout[mine, t].astype(jnp.float32) + arrived).astype(narrow)
        for n, m in enumerate(own_list):
            if m[0] >= split:
                over_tiles(m[0], m[1], step)
                y_copy(n).start()

    def forward_all(i, joined):
        for n in range(len(list_of(i))):
            forward(i, n, joined)

    @pl.when(edge)
    def _():
        if short:
            with jax.named_scope("edge_first"):
                forward_all(0, False)
                merge()
            with jax.named_scope("edge_middle"):
                forward_all(1, False)
            with jax.named_scope("edge_last"):
                for n in range(len(lists[2])):
                    forward(2, n, False, crossed=n < 2)
        else:
            loop(0, planes - 1, lambda i: forward_all(i, False))

    @pl.when(jnp.logical_not(edge))
    def _():
        if short:
            with jax.named_scope("inner_first"):
                forward_all(0, True)
                merge()
            with jax.named_scope("inner_both"):
                forward(1, 0, True)
                for n, m in enumerate(lists[0]):
                    z_wait(plane(2), m, n)
                forward(2, 2, True, crossed=False, wait=False)
                forward(1, 1, True)
                forward(2, 3, True, crossed=False, wait=False)
                forward(1, 2, True)
                forward(2, 0, True, wait=False)
                forward(1, 3, True)
                forward(2, 1, True, wait=False)
        else:
            loop(0, planes - 1, lambda i: forward_all(i, True))

    small[3].wait()
    swap.wait_send()
    pltpu.make_async_remote_copy(
        src_ref=dout, dst_ref=dgot, send_sem=dsend, recv_sem=srecv, device_id=pair, device_id_type=MESH,
    ).wait_send()

    held = {False: 0, True: 0}

    def arrive(stop):
        beyond = mine + (1 - mine % 2) * (planes - mine)
        for far, group in ((False, lists[-1]), (True, lists[-2])):
            at = mine + planes - beyond if far else beyond
            done = sorted(range(len(group)), key=lambda n: group[n][0])
            while held[far] < len(done) and group[done[held[far]]][0] < stop:
                n = done[held[far]]
                held[far] += 1
                if far:
                    pl.when(jnp.logical_not(edge))(functools.partial(z_wait, at, group[n], n))
                elif short:
                    z_wait(at, group[n], n)
                else:
                    pl.when(jnp.logical_or(jnp.logical_not(edge), beyond == planes * (1 - up) + mine * up))(
                        functools.partial(z_wait, at, group[n], n))

    for n, (start, many) in enumerate(own_list):
        with jax.named_scope("finish_x"):
            y_copy(n).wait_recv()
        with jax.named_scope("finish_z"):
            arrive(start + many)
        with jax.named_scope("finish"):
            found = []
            for t in range(start, start + many):
                total = cell(mine, t, 0, share) + xgot[mine, t].astype(jnp.float32)
                total = total + zgot[mine, t].astype(jnp.float32) + zgot[planes, t].astype(jnp.float32)
                found.append(total.astype(jnp.bfloat16))
            done = jnp.dot(jnp.concatenate(found, axis=0), kern_v[...], preferred_element_type=jnp.float32)
            for u in range(many):
                out[:, start + u, :] = done[u * share:(u + 1) * share]
    with jax.named_scope("leave"):
        pltpu.make_async_remote_copy(
            src_ref=xout, dst_ref=xgot, send_sem=xsend, recv_sem=srecv, device_id=across, device_id_type=MESH,
        ).wait_send()
        pltpu.make_async_remote_copy(
            src_ref=xgot.at[0:planes - 1], dst_ref=zgot.at[0:planes - 1], send_sem=zsend, recv_sem=srecv,
            device_id=beside, device_id_type=MESH,
        ).wait_send()


def exchange(bins, spots, vis, rows, cols, kern, planes, tiles):
    count, fold, _, share, width = rows.shape
    wide = 2 * cols.shape[2]
    lists, near, own_list, split = messages(planes, tiles, share)
    any_spec = pl.BlockSpec(memory_space=pltpu.HBM)
    half = jnp.bfloat16
    dma = pltpu.SemaphoreType.DMA
    table = (-(-(1 + -(-planes * tiles // 128)) // 8) * 8, 128)
    grids = (2 * planes + planes + 1 + 2) * tiles * share * wide * 2
    held = 2 * (rows.size + cols.size + kern.size) + 8 * (count + 1) * share * wide + 8 * count * share * wide
    limit = min(LIMIT, grids + held + 6 * 1024 * 1024)
    operands = [pltpu.with_memory_space_constraint(a, pltpu.HBM) for a in (bins, spots, vis, rows, cols, kern)]
    return pl.pallas_call(
        functools.partial(exchange_kernel, planes, tiles),
        out_shape=jax.ShapeDtypeStruct((share, tiles, wide), jnp.float32),
        in_specs=[any_spec] * 6,
        out_specs=pl.BlockSpec(memory_space=pltpu.VMEM),
        scratch_shapes=[
            pltpu.VMEM(bins.shape, jnp.int32),
            pltpu.VMEM(spots.shape, jnp.int32),
            pltpu.SMEM((2,) + table, jnp.int32),
            pltpu.VMEM((2,) + table, jnp.int32),
            pltpu.VMEM(vis.shape, vis.dtype),
            pltpu.VMEM(rows.shape, rows.dtype),
            pltpu.VMEM(cols.shape, cols.dtype),
            pltpu.VMEM(kern.shape, kern.dtype),
            pltpu.VMEM((2, count + 1, share, wide), jnp.float32),
            pltpu.VMEM((2, 2, count, share, wide // 2), half),
            pltpu.VMEM((2, 2, count, share, wide // 2), half),
            pltpu.VMEM((planes, tiles, share, wide), half),
            pltpu.VMEM((planes, tiles, share, wide), half),
            pltpu.VMEM((planes + 1, tiles, share, wide), half),
            pltpu.VMEM((max(tiles - split, 1), share, wide), half),
            dma((6,)),
            dma((2, PIECES)),
            dma,
            dma,
            dma,
            dma((6,)),
            dma,
            dma((planes - 1, 4)),
            dma((len(own_list),)),
            dma,
            dma((planes + 1, 4)),
            dma((2,)),
        ],
        compiler_params=pltpu.CompilerParams(
            collective_id=0, has_side_effects=True, vmem_limit_bytes=limit
        ),
        name="exchange",
    )(*operands)


def body(vis, row_weight, col_weight, w_bin, tile_col, w_kernel):
    planes = lax.axis_size("tm")
    chans = lax.axis_size("chan")
    count, rows_k, width_v = row_weight.shape[1:]
    tile_count = GC // QW
    fold = chans // 2
    bins = w_bin.reshape(1, count)
    rows = row_weight[0].reshape(count, fold, 2, rows_k // chans, width_v)
    result = exchange(bins, tile_col, vis[0], rows, col_weight[0], w_kernel[0], planes, tile_count)
    return result[None]


def solution(mesh):
    in_specs = (
        P(("groups", "chan"), "tm", None, None),
        P(("groups", "chan"), "tm", None, None),
        P(("groups", "chan"), "tm", None, None),
        P(("groups", "chan"), "tm", None),
        P(("groups", "chan"), "tm"),
        P(("groups", "tm"), None, None),
    )
    out_specs = P(("groups", "tm"), "chan", None, None)
    return jax.shard_map(body, mesh=mesh, in_specs=in_specs, out_specs=out_specs, check_vma=False)
```

```python
import functools
import jax
import jax.numpy as jnp
from jax import lax
from jax.experimental import pallas as pl
from jax.experimental.pallas import tpu as pltpu
from jax.sharding import PartitionSpec as P

QW = 256
GC = 4096
MESH = pl.DeviceIdType.MESH
LIMIT = 63 * 1024 * 1024
PIECES = 2
NEAR = 9


def write_table(table, bins, spots, cells, tiles):
    count = bins.shape[1]
    down = lax.broadcasted_iota(jnp.int32, (count, count), 0)
    along = lax.broadcasted_iota(jnp.int32, (count, count), 1)
    flat = jnp.broadcast_to(bins * tiles + spots, (count, count))
    tall = jnp.max(jnp.where(down == along, flat, 0), axis=1, keepdims=True)
    before = jnp.max(jnp.where((tall == flat) & (down < along), down + 1, 0), axis=0, keepdims=True)
    table[...] = jnp.zeros(table.shape, jnp.int32)
    table[0:1, 0:count] = before
    deep = lax.broadcasted_iota(jnp.int32, (count, 128), 0)
    wide = lax.broadcasted_iota(jnp.int32, (count, 128), 1)
    for r in range(-(-cells // 128)):
        named = tall == wide + r * 128
        table[1 + r:2 + r, :] = jnp.max(jnp.where(named, deep + 1, 0), axis=0, keepdims=True)


def loop(start, stop, step):
    def body(i, carry):
        step(i)
        return carry
    lax.fori_loop(start, stop, body, 0)


def messages(planes, tiles, share):
    quarter, half = tiles // 4, share // 2
    even = [(q * quarter, quarter, 0, share) for q in range(4)]
    if planes != 4:
        own = [(t, 2) for t in range(0, tiles, 2)]
        return [even] * (planes - 1), [], own, tiles
    split = tiles - NEAR
    first = [(t, tiles // 2, r, half) for r in (0, half) for t in (tiles // 2, 0)]
    last = [(0, quarter, 0, share), (quarter, split - quarter, 0, share)]
    last += [(split, NEAR - 2, 0, share), (tiles - 2, 2, 0, share)]
    near = [(split, NEAR, r, half) for r in (0, half)]
    own = [(t, min(2, split - t)) for t in range(0, split, 2)]
    own += [(t, 2) for t in range(split, tiles - 5, 2)]
    at = own[-1][0] + own[-1][1]
    own += [(at, tiles - 2 - at), (tiles - 2, 2)]
    return [first, even, last], near, own, split


def exchange_kernel(
    planes, tiles, bins, spots, vis, rows, cols, kern, out,
    bins_v, spots_v, tab_s, tab_v, vis_v, rows_v, cols_v, kern_v, runs, pairs, dout, dgot, xout, xgot, zgot, ngot,
    lsem, psem, ssend, srecv, dsend, drecv, xsend, xrecv, yrecv, zsend, zrecv, nrecv,
):
    me, mine = lax.axis_index("chan"), lax.axis_index("tm")
    core, row = me % 2, me // 2
    pair = {"chan": row * 2 + 1 - core}
    across = {"chan": (1 - row) * 2 + core}
    count, share = rows_v.shape[0], rows_v.shape[3]
    half_rows = share // 2
    piece = count // PIECES
    narrow = xout.dtype
    edge = mine % (planes - 1) == 0
    up = mine // (planes // 2)
    reach = up * mine + (1 - up) * (planes - 1 - mine)
    beside = {"tm": mine + 1 - 2 * (mine % 2)}
    lists, near, own_list, split = messages(planes, tiles, share)
    short = len(near) > 0

    def less(a, b):
        return (planes - 1 + b - a) // planes

    def plane(i):
        late = i // reach
        v = (1 - late) * i + late * (planes - 1 - (i - reach))
        return up * v + (1 - up) * (planes - 1 - v)

    def slot(w):
        return w + less(w, mine) * (1 - less(w, mine - 1)) * (planes - w)

    def list_of(i):
        return lists[i] if short else lists[0]

    small = [
        pltpu.make_async_copy(src, dst, lsem.at[i])
        for i, (src, dst) in enumerate(((bins, bins_v), (spots, spots_v), (vis, vis_v), (kern, kern_v)))
    ]
    parts = []
    for p in range(PIECES):
        cut = pl.ds(p * piece, piece)
        parts.append([
            pltpu.make_async_copy(rows.at[cut], rows_v.at[cut], psem.at[0, p]),
            pltpu.make_async_copy(cols.at[cut], cols_v.at[cut], psem.at[1, p]),
        ])
    for copy in small[:3] + sum(parts, []) + small[3:]:
        copy.start()

    barrier = pltpu.get_barrier_semaphore()
    pl.semaphore_signal(barrier, inc=1, device_id=pair, device_id_type=MESH)
    pl.semaphore_signal(barrier, inc=1, device_id=across, device_id_type=MESH)

    def greet(step):
        pl.semaphore_signal(barrier, inc=1, device_id={"tm": mine + step}, device_id_type=MESH)
    pl.when(mine > 0)(lambda: greet(-1))
    pl.when(mine < planes - 1)(lambda: greet(1))

    table = pltpu.make_async_copy(tab_v, tab_s.at[0], lsem.at[4])
    swap = pltpu.make_async_remote_copy(
        src_ref=tab_v, dst_ref=tab_s.at[1], send_sem=ssend, recv_sem=srecv, device_id=pair, device_id_type=MESH,
    )
    runs[0] = jnp.zeros(runs.shape[1:], runs.dtype)
    pairs[0] = jnp.zeros(pairs.shape[1:], pairs.dtype)

    @pl.when(edge)
    def _():
        zgot[(mine // (planes - 1)) * planes] = jnp.zeros(zgot.shape[1:], narrow)

    def entry(s, i):
        return tab_s[s, i // 128, i % 128]

    def d_copy(r, p):
        cut = pl.ds(p * (count // 2), count // 2)
        return pltpu.make_async_remote_copy(
            src_ref=dout.at[0, r, cut], dst_ref=dgot.at[0, r, cut], send_sem=dsend, recv_sem=drecv.at[2 * r + p],
            device_id=pair, device_id_type=MESH,
        )

    def e_copy(p):
        cut = pl.ds(p * (count // 2), count // 2)
        return pltpu.make_async_remote_copy(
            src_ref=dout.at[1, :, cut], dst_ref=dgot.at[1, :, cut], send_sem=dsend, recv_sem=drecv.at[4 + p],
            device_id=pair, device_id_type=MESH,
        )

    def build_other(s, x, p):
        for b in range(p * piece, (p + 1) * piece):
            other = rows_v[b, x, 1 - core]
            real, imag = vis_v[b, 0:1, :], vis_v[b, 1:2, :]
            upper, lower = other[:half_rows], other[half_rows:]
            weighted = jnp.concatenate([upper * real, upper * imag, lower * real, lower * imag], axis=0)
            found = jnp.dot(weighted, cols_v[b], preferred_element_type=jnp.float32).astype(narrow)
            dout[s, 0, b] = found[:share]
            dout[s, 1, b] = found[share:]

    def build_own(x, p):
        for b in range(p * piece, (p + 1) * piece):
            own = rows_v[b, x, core]
            real, imag = vis_v[b, 0:1, :], vis_v[b, 1:2, :]
            weighted = jnp.concatenate([own * real, own * imag], axis=0)
            found = jnp.dot(weighted, cols_v[b], preferred_element_type=jnp.float32)
            runs[b + 1, :, 0:QW] = found[:share]
            runs[b + 1, :, QW:2 * QW] = found[share:]

    batch = 4 if count % 8 == 0 else 1

    def join(s, r, p):
        low, high = r * half_rows, (r + 1) * half_rows

        def step(i):
            for u in range(batch):
                b = p * (count // 2) + i * batch + u
                found, own, last = dgot[s, r, b].astype(jnp.float32), entry(0, b), entry(1, b)
                runs[b + 1, low:high] = runs[b + 1, low:high] + runs[own, low:high]
                pairs[b + 1, low:high, 0:QW] = found[:half_rows] + pairs[last, low:high, 0:QW]
                pairs[b + 1, low:high, QW:2 * QW] = found[half_rows:] + pairs[last, low:high, QW:2 * QW]
        loop(0, count // 2 // batch, step)

    def cell(w, t, low, high):
        i = 128 + w * tiles + t
        return runs[entry(0, i), low:high] + pairs[entry(1, i), low:high]

    def window(ref, w, m):
        start, many, low, deep = m
        return ref.at[w, start:start + many, low:low + deep]

    def x_copy(i, n):
        w, m = plane(i), list_of(i)[n]
        return pltpu.make_async_remote_copy(
            src_ref=window(xout, w, m), dst_ref=window(xgot, w, m),
            send_sem=xsend, recv_sem=xrecv.at[i, n], device_id=across, device_id_type=MESH,
        )

    def y_copy(n):
        m = own_list[n] + (0, share)
        return pltpu.make_async_remote_copy(
            src_ref=window(xout, mine, m), dst_ref=window(xgot, mine, m),
            send_sem=xsend, recv_sem=yrecv.at[n], device_id=across, device_id_type=MESH,
        )

    def z_copy(i, n):
        w, m = plane(i), list_of(i)[n]
        return pltpu.make_async_remote_copy(
            src_ref=window(xgot, w, m), dst_ref=window(zgot, slot(w), m),
            send_sem=zsend, recv_sem=zrecv.at[slot(w), n],
            device_id={"tm": mine + 2 * less(mine, w) - 1}, device_id_type=MESH,
        )

    def z_wait(at, m, n):
        pltpu.make_async_remote_copy(
            src_ref=window(xgot, 0, m), dst_ref=window(zgot, at, m),
            send_sem=zsend, recv_sem=zrecv.at[at, n], device_id=beside, device_id_type=MESH,
        ).wait_recv()

    def near_copy(n):
        start, many, low, deep = near[n]
        return pltpu.make_async_remote_copy(
            src_ref=window(xout, plane(planes - 2), near[n]), dst_ref=ngot.at[:, low:low + deep],
            send_sem=xsend, recv_sem=nrecv.at[n], device_id=beside, device_id_type=MESH,
        )

    def over_tiles(start, many, step):
        pairs = many // 2

        def two(i):
            step(start + 2 * i)
            step(start + 2 * i + 1)
        loop(0, pairs, two)
        if many % 2:
            step(start + many - 1)

    def fill(w, m):
        start, many, low, deep = m

        def step(t):
            xout[w, t, low:low + deep] = cell(w, t, low, low + deep).astype(narrow)
        over_tiles(start, many, step)

    def send(i, n):
        fill(plane(i), list_of(i)[n])
        x_copy(i, n).start()

    def approach(n):
        fill(plane(planes - 2), near[n])
        near_copy(n).start()

    with jax.named_scope("table"):
        for copy in small[:2]:
            copy.wait()
        write_table(tab_v, bins_v[...], spots_v[...], planes * tiles, tiles)
        table.start()
    with jax.named_scope("vis_wait"):
        small[2].wait()
    for p in range(PIECES):
        with jax.named_scope("load_wait"):
            for copy in parts[p]:
                copy.wait()
        with jax.named_scope("build_other"):
            build_other(0, 1 - row, p)
        if p == 0:
            with jax.named_scope("barrier"):
                pl.semaphore_wait(barrier, 3 + less(0, mine) * less(mine, planes - 1))
            swap.start()
        d_copy(0, p).start()
    for p in range(PIECES):
        d_copy(1, p).start()
    for p in range(PIECES):
        with jax.named_scope("build_own"):
            build_own(1 - row, p)
    with jax.named_scope("swap_wait"):
        swap.wait_recv()
        table.wait()
    for p in range(2):
        with jax.named_scope("pair_wait"):
            d_copy(0, p).wait_recv()
        with jax.named_scope("join_far"):
            join(0, 0, p)
    if short:
        with jax.named_scope("fill_first"):
            send(0, 0)
            approach(0)
            send(0, 1)
    for p in range(2):
        with jax.named_scope("pair_wait"):
            d_copy(1, p).wait_recv()
        with jax.named_scope("join_far"):
            join(0, 1, p)
    with jax.named_scope("fill"):
        if short:
            send(0, 2)
            send(0, 3)
            approach(1)
            for n in range(len(lists[1])):
                send(1, n)
            for n in range(2):
                send(2, n)
        else:
            def send_all(i):
                for n in range(len(list_of(i))):
                    send(i, n)
            loop(0, planes - 1, send_all)
        for n, m in enumerate(own_list):
            fill(mine, m + (0, share))
            if m[0] < split:
                y_copy(n).start()

    for p in range(PIECES):
        with jax.named_scope("build_near"):
            build_other(1, row, p)
        e_copy(p).start()
    for p in range(PIECES):
        with jax.named_scope("build_near"):
            build_own(row, p)
    for p in range(2):
        with jax.named_scope("join_near"):
            e_copy(p).wait_recv()
            join(1, 0, p)
            join(1, 1, p)

    def gather(w, m, crossed, joined):
        start, many, low, deep = m
        high = low + deep

        def step(t):
            total = cell(w, t, low, high)
            if crossed:
                total = total + xgot[w, t, low:high].astype(jnp.float32)
            if joined:
                total = total + zgot[w, t, low:high].astype(jnp.float32)
            xgot[w, t, low:high] = total.astype(narrow)
        over_tiles(start, many, step)

    def forward(i, n, joined, crossed=True, wait=True):
        w, m = plane(i), list_of(i)[n]
        if crossed:
            x_copy(i, n).wait_recv()
        if joined and wait:
            z_wait(w, m, n)
        gather(w, m, crossed, joined)
        z_copy(i, n).start()

    def merge():
        for n in range(len(near)):
            near_copy(n).wait_recv()

        def step(t):
            arrived = ngot[t - split].astype(jnp.float32)
            xout[mine, t] = (xout[mine, t].astype(jnp.float32) + arrived).astype(narrow)
        for n, m in enumerate(own_list):
            if m[0] >= split:
                over_tiles(m[0], m[1], step)
                y_copy(n).start()

    def forward_all(i, joined):
        for n in range(len(list_of(i))):
            forward(i, n, joined)

    @pl.when(edge)
    def _():
        if short:
            with jax.named_scope("edge_first"):
                forward_all(0, False)
                merge()
            with jax.named_scope("edge_middle"):
                forward_all(1, False)
            with jax.named_scope("edge_last"):
                for n in range(len(lists[2])):
                    forward(2, n, False, crossed=n < 2)
        else:
            loop(0, planes - 1, lambda i: forward_all(i, False))

    @pl.when(jnp.logical_not(edge))
    def _():
        if short:
            with jax.named_scope("inner_first"):
                forward_all(0, True)
                merge()
            with jax.named_scope("inner_both"):
                forward(1, 0, True)
                for n, m in enumerate(lists[0]):
                    z_wait(plane(2), m, n)
                forward(2, 2, True, crossed=False, wait=False)
                forward(1, 1, True)
                forward(2, 3, True, crossed=False, wait=False)
                forward(1, 2, True)
                forward(2, 0, True, wait=False)
                forward(1, 3, True)
                forward(2, 1, True, wait=False)
        else:
            loop(0, planes - 1, lambda i: forward_all(i, True))

    small[3].wait()
    swap.wait_send()
    pltpu.make_async_remote_copy(
        src_ref=dout, dst_ref=dgot, send_sem=dsend, recv_sem=srecv, device_id=pair, device_id_type=MESH,
    ).wait_send()

    held = {False: 0, True: 0}

    def arrive(stop):
        beyond = mine + (1 - mine % 2) * (planes - mine)
        for far, group in ((False, lists[-1]), (True, lists[-2])):
            at = mine + planes - beyond if far else beyond
            done = sorted(range(len(group)), key=lambda n: group[n][0])
            while held[far] < len(done) and group[done[held[far]]][0] < stop:
                n = done[held[far]]
                held[far] += 1
                if far:
                    pl.when(jnp.logical_not(edge))(functools.partial(z_wait, at, group[n], n))
                elif short:
                    z_wait(at, group[n], n)
                else:
                    pl.when(jnp.logical_or(jnp.logical_not(edge), beyond == planes * (1 - up) + mine * up))(
                        functools.partial(z_wait, at, group[n], n))

    for n, (start, many) in enumerate(own_list):
        with jax.named_scope("finish_x"):
            y_copy(n).wait_recv()
        with jax.named_scope("finish_z"):
            arrive(start + many)
        with jax.named_scope("finish"):
            found = []
            for t in range(start, start + many):
                total = cell(mine, t, 0, share) + xgot[mine, t].astype(jnp.float32)
                total = total + zgot[mine, t].astype(jnp.float32) + zgot[planes, t].astype(jnp.float32)
                found.append(total.astype(jnp.bfloat16))
            done = jnp.dot(jnp.concatenate(found, axis=0), kern_v[...], preferred_element_type=jnp.float32)
            for u in range(many):
                out[:, start + u, :] = done[u * share:(u + 1) * share]
    with jax.named_scope("leave"):
        pltpu.make_async_remote_copy(
            src_ref=xout, dst_ref=xgot, send_sem=xsend, recv_sem=srecv, device_id=across, device_id_type=MESH,
        ).wait_send()
        pltpu.make_async_remote_copy(
            src_ref=xgot.at[0:planes - 1], dst_ref=zgot.at[0:planes - 1], send_sem=zsend, recv_sem=srecv,
            device_id=beside, device_id_type=MESH,
        ).wait_send()


def exchange(bins, spots, vis, rows, cols, kern, planes, tiles):
    count, fold, _, share, width = rows.shape
    wide = 2 * cols.shape[2]
    lists, near, own_list, split = messages(planes, tiles, share)
    any_spec = pl.BlockSpec(memory_space=pltpu.HBM)
    half = jnp.bfloat16
    dma = pltpu.SemaphoreType.DMA
    table = (-(-(1 + -(-planes * tiles // 128)) // 8) * 8, 128)
    grids = (2 * planes + planes + 1 + 2) * tiles * share * wide * 2
    held = 2 * (rows.size + cols.size + kern.size) + 8 * (count + 1) * share * wide + 8 * count * share * wide
    limit = min(LIMIT, grids + held + 6 * 1024 * 1024)
    operands = [pltpu.with_memory_space_constraint(a, pltpu.HBM) for a in (bins, spots, vis, rows, cols, kern)]
    return pl.pallas_call(
        functools.partial(exchange_kernel, planes, tiles),
        out_shape=jax.ShapeDtypeStruct((share, tiles, wide), jnp.float32),
        in_specs=[any_spec] * 6,
        out_specs=pl.BlockSpec(memory_space=pltpu.VMEM),
        scratch_shapes=[
            pltpu.VMEM(bins.shape, jnp.int32),
            pltpu.VMEM(spots.shape, jnp.int32),
            pltpu.SMEM((2,) + table, jnp.int32),
            pltpu.VMEM(table, jnp.int32),
            pltpu.VMEM(vis.shape, vis.dtype),
            pltpu.VMEM(rows.shape, rows.dtype),
            pltpu.VMEM(cols.shape, cols.dtype),
            pltpu.VMEM(kern.shape, kern.dtype),
            pltpu.VMEM((count + 1, share, wide), jnp.float32),
            pltpu.VMEM((count + 1, share, wide), jnp.float32),
            pltpu.VMEM((2, 2, count, share, wide // 2), half),
            pltpu.VMEM((2, 2, count, share, wide // 2), half),
            pltpu.VMEM((planes, tiles, share, wide), half),
            pltpu.VMEM((planes, tiles, share, wide), half),
            pltpu.VMEM((planes + 1, tiles, share, wide), half),
            pltpu.VMEM((max(tiles - split, 1), share, wide), half),
            dma((5,)),
            dma((2, PIECES)),
            dma,
            dma,
            dma,
            dma((6,)),
            dma,
            dma((planes - 1, 4)),
            dma((len(own_list),)),
            dma,
            dma((planes + 1, 4)),
            dma((2,)),
        ],
        compiler_params=pltpu.CompilerParams(
            collective_id=0, has_side_effects=True, vmem_limit_bytes=limit
        ),
        name="exchange",
    )(*operands)


def body(vis, row_weight, col_weight, w_bin, tile_col, w_kernel):
    planes = lax.axis_size("tm")
    chans = lax.axis_size("chan")
    count, rows_k, width_v = row_weight.shape[1:]
    tile_count = GC // QW
    fold = chans // 2
    bins = w_bin.reshape(1, count)
    rows = row_weight[0].reshape(count, fold, 2, rows_k // chans, width_v)
    result = exchange(bins, tile_col, vis[0], rows, col_weight[0], w_kernel[0], planes, tile_count)
    return result[None]


def solution(mesh):
    in_specs = (
        P(("groups", "chan"), "tm", None, None),
        P(("groups", "chan"), "tm", None, None),
        P(("groups", "chan"), "tm", None, None),
        P(("groups", "chan"), "tm", None),
        P(("groups", "chan"), "tm"),
        P(("groups", "tm"), None, None),
    )
    out_specs = P(("groups", "tm"), "chan", None, None)
    return jax.shard_map(body, mesh=mesh, in_specs=in_specs, out_specs=out_specs, check_vma=False)
```
